512 devices in a mesh: cls: 32 (over z, x_hi, core), dp: 16 (over y, x_lo).
Axes of the slice: x: 4 (x_hi: 2, x_lo: 2; x = x_hi * 2 + x_lo), y: 8, z: 8, core: 2. Of those that a mesh axis runs over, the one named last changes fastest.
Arguments:
- hidden: bfloat16 [320, 3072], P('dp'), may hold values from -7 to 7
- weight: bfloat16 [196608, 3072], P(('cls', 'dp')), may hold values from -8 to 8
- labels: int32 [320], replicated, may hold values from 0 to 196607
- cotangent: float32 [320], replicated, may hold values from -4 to 4
Outputs:
- token_loss: float32 [320], P('dp')
- weight_grad: bfloat16 [196608, 3072], P(('cls', 'dp'))
- hidden_grad: bfloat16 [320, 3072], P('dp', 'cls')
The draws below stay inside these ranges and needn't reach their ends.
All inputs are finite; a program needn't handle non-finite values.
Results may differ from the reference program's by a relative error of at most 0.0049.
Values may be sent and summed in bfloat16 or wider, within the bound.
A program may use at most 64 MiB of HBM per device.

```python
import math
import jax
import jax.numpy as jnp
import numpy as np
from jax import lax

D = 3072
V = 196608
TOKENS = 320


def base_states(key):
    values_key = jax.random.fold_in(key, 11)
    states = jnp.clip(jax.random.normal(values_key, (TOKENS, D), jnp.float32), -6.0, 6.0)
    return states


def draw_hidden(key, part):
    return base_states(key).astype(jnp.bfloat16)


def draw_weight(key, part):
    raw = jax.random.normal(jax.random.fold_in(key, 21), (V, D), jnp.float32)
    ramp = (2.5 + 0.7 * jnp.arange(V, dtype=jnp.float32) / V) / math.sqrt(D)
    table = jnp.clip(raw * ramp[:, None], -0.5, 0.5)
    return table.astype(jnp.bfloat16)


def set_ends(entries, key, least, high):
    shape = entries.shape
    spot = [jax.random.randint(jax.random.fold_in(key, axis), (), 0, shape[axis]) for axis in range(len(shape))]
    entries = entries.at[tuple(spot)].set(least)
    longest = shape.index(max(shape))
    spot[longest] = (spot[longest] + 1) % shape[longest]
    return entries.at[tuple(spot)].set(high)


def skewed_wide(rng, extent, count, skew):
    weights = [min(1 << octave, count + 1 - (1 << octave)) * (1 << 20) // math.isqrt((1 << octave) ** skew) + 1 for octave in range((count + 1).bit_length()) if 1 << octave <= count]
    spread = 1 + sum(weights) // (1 << 30)
    grid = np.cumsum(np.array([max(1, weight // spread) for weight in weights]))
    ticket = jax.random.randint(jax.random.fold_in(rng, 1), extent, 0, int(grid[len(weights) - 1]))
    start = jnp.left_shift(1, jnp.searchsorted(jnp.asarray(grid, jnp.int32), ticket, side="right").astype(jnp.int32))
    rank = start - 1 + jax.random.randint(jax.random.fold_in(rng, 4), extent, 0, 1 << 30) % jnp.minimum(start, count + 1 - start)
    return jax.random.permutation(jax.random.fold_in(rng, 2), count)[rank].astype(jnp.int32)


def normal_values(rng, shape, spread, bound, kind=jnp.bfloat16):
    drawn = jax.random.normal(rng, shape, jnp.float32) * spread
    return jnp.minimum(jnp.maximum(drawn, -bound), bound).astype(kind)


def setup_inputs(seed: int = 0) -> dict:
    key_of = jax.random.split(jax.random.key(seed), 5)
    return {
        "hidden": draw_hidden(jax.random.fold_in(key_of[4], 71), 0),
        "weight": draw_weight(jax.random.fold_in(key_of[4], 71), 0),
        "labels": set_ends(skewed_wide(key_of[2], (TOKENS,), V, 2), jax.random.fold_in(key_of[2], 3), 0, V - 1).astype(jnp.int32),
        "cotangent": normal_values(key_of[3], (TOKENS,), 1.0, 4.0, jnp.float32),
    }


def reference(hidden, weight, labels, cotangent):
    logits = lax.dot_general(hidden, weight, (((1,), (1,)), ((), ())), preferred_element_type=jnp.float32)
    peak = jnp.max(logits, axis=1)
    shifted = jnp.exp(logits - peak[:, None])
    total = jnp.sum(shifted, axis=1)
    columns = lax.broadcasted_iota(jnp.int32, logits.shape, 1)
    chosen = columns == labels.astype(jnp.int32)[:, None]
    picked = jnp.sum(jnp.where(chosen, logits, jnp.zeros_like(logits)), axis=1)
    token_loss = peak + jnp.log(total) - picked
    softmax_vals = shifted / total[:, None]
    grad_logits = (cotangent[:, None] * (softmax_vals - chosen.astype(jnp.float32))).astype(jnp.bfloat16)
    weight_grad = lax.dot_general(grad_logits, hidden, (((0,), (0,)), ((), ())), preferred_element_type=jnp.float32).astype(jnp.bfloat16)
    hidden_grad = jnp.dot(grad_logits, weight, preferred_element_type=jnp.float32).astype(jnp.bfloat16)
    return (token_loss, weight_grad, hidden_grad)
```

```python
import jax
import jax.numpy as jnp
from jax import lax
from jax.experimental import pallas as pl
from jax.experimental.pallas import tpu as pltpu
from jax.sharding import Mesh
from jax.sharding import PartitionSpec as P

CLS = ("cls_0", "cls_1", "cls_2")
DP = ("dp_0", "dp_1")
CLS_DP = ("cls_0", "cls_1", "cls_2", "dp_0", "dp_1")
MESH = pl.DeviceIdType.MESH
F32 = jnp.float32
BF16 = jnp.bfloat16

RING = 8
SHARDS = 16
D = 3072
ROWS = 384
TOK = 320
MAIN = 256
REST = 64
HALF = D // 2
PACK = HALF + HALF // 4
SUB = ((0, 1024), (1024, PACK - 1024))
BLK = 384
RIGHT = RING // 2
LEFT = RING - 1 - RIGHT
ORDER = (4, 5, 3, 6, 2, 7, 1, 0)


def nt(a, b):
    return lax.dot_general(a, b, (((1,), (1,)), ((), ())), preferred_element_type=F32)


def tn(a, b):
    return lax.dot_general(a, b, (((0,), (0,)), ((), ())), preferred_element_type=F32)


def nn(a, b):
    return lax.dot_general(a, b, (((1,), (0,)), ((), ())), preferred_element_type=F32)


def kernel(
    hid, w_hbm, labels, cot, loss_out, wg_out, hg_out,
    w, g, xr, lt, gt, stat_send, stat_recv, pb, rb, send_r, send_l, recv_r, recv_l,
    f32buf, f_send, f_recv, s_send, s_recv, wg,
    w_sem, wg_sem, ring_s, ring_v, x_s, x_v, d_s, d_v, st_s, st_v, c_s, c_v, rr_s, rr_v, f_s, f_v, e_s, e_v,
):
    z, xh, c = lax.axis_index("cls_0"), lax.axis_index("cls_1"), lax.axis_index("cls_2")
    y, xl = lax.axis_index("dp_0"), lax.axis_index("dp_1")
    x = xh * 2 + xl
    me = y * 2 + xl

    def at_y(d):
        return {"dp_0": (y + d) % RING}

    def at_z(d):
        return {"cls_0": (z + d) % RING}

    def at_x(dx, dc):
        there = (x + dx) % 4
        return {"cls_1": there // 2, "dp_1": there % 2, "cls_2": (c + dc) % 2}

    partner = {"cls_2": 1 - c}

    def copy(src, dst, s, v, device):
        return pltpu.make_async_remote_copy(
            src_ref=src, dst_ref=dst, send_sem=s, recv_sem=v, device_id=device, device_id_type=MESH
        )

    load_w = pltpu.make_async_copy(w_hbm, w, w_sem)
    load_w.start()

    barrier = pltpu.get_barrier_semaphore()
    others = [(dx, dc) for dx in range(4) for dc in range(2) if dx or dc]
    peers = [at_x(dx, dc) for dx, dc in others]
    peers += [at_y(d) for d in range(1, RING)] + [at_z(d) for d in range(1, RING)]
    for peer in peers:
        pl.semaphore_signal(barrier, inc=1, device_id=peer, device_id_type=MESH)
    pl.semaphore_wait(barrier, len(peers))

    sent = []

    def shard(o, own):
        return ((y + o) % RING) * 2 + (xl if own else 1 - xl)

    def part(o, own, h, sub):
        return g.at[shard(o, own), h, :, pl.ds(*SUB[sub])]

    def begin(d):
        d.start()
        sent.append(d)

    def source(o, sub):
        return hid.at[c, :, pl.ds(*SUB[sub])] if o == 0 else part(o, True, c, sub)

    def ring(side, step, sub):
        o = -step if side == 0 else step
        begin(copy(source(o, sub), part(o, True, c, sub), ring_s.at[side, step, sub],
                   ring_v.at[side, step, sub], at_y(1 if side == 0 else -1)))

    def spread_x(o, sub):
        begin(copy(source(o, sub), part(o, True, c, sub), x_s.at[o % RING, sub],
                   x_v.at[o % RING, sub], at_x(1 if sub == 0 else 3, 0)))

    def spread_core(o, own, sub):
        begin(copy(part(o, own, c, sub), part(o, own, c, sub), d_s.at[o % RING, int(own), sub],
                   d_v.at[o % RING, int(own), sub], partner))

    def arrived(ref, s, v):
        copy(ref, ref, s, v, partner).wait_recv()

    for sub in range(2):
        ring(0, 0, sub)
        ring(1, 0, sub)
        spread_x(0, sub)
    g[me] = hid[...]

    def from_x(o):
        for sub in range(2):
            arrived(part(o, False, c, sub), x_s.at[o % RING, sub], x_v.at[o % RING, sub])
            spread_core(o, False, sub)

    waiting = [0]
    for step in range(RIGHT):
        got = []
        for sub in range(2):
            for side in range(2):
                if side == 1 and step >= LEFT:
                    continue
                o = -(step + 1) if side == 0 else step + 1
                arrived(part(o, True, c, sub), ring_s.at[side, step, sub], ring_v.at[side, step, sub])
                if step + 1 < (RIGHT if side == 0 else LEFT):
                    ring(side, step + 1, sub)
                spread_x(o, sub)
                spread_core(o, True, sub)
                if sub == 1:
                    got.append(o)
        for o in waiting:
            from_x(o)
        waiting = got
    for o in waiting:
        from_x(o)
    for o in [0] + [k for step in range(RIGHT) for k in (-(step + 1), step + 1)][: RING - 1]:
        for own in (True, False):
            if o == 0 and own:
                continue
            for sub in range(2):
                arrived(part(o, own, 1 - c, sub), d_s.at[o % RING, int(own), sub], d_v.at[o % RING, int(own), sub])
    load_w.wait()

    to = lax.broadcasted_iota(jnp.int32, (MAIN, MAIN), 0)
    source_row = lax.broadcasted_iota(jnp.int32, (MAIN, MAIN), 1)
    perm = (source_row == ((to & 63) >> 2) * 16 + (to >> 6) * 4 + (to & 3)).astype(F32).astype(BF16)
    col = lax.broadcasted_iota(jnp.int32, (BLK, 512), 0)
    lane = lax.broadcasted_iota(jnp.int32, (BLK, 512), 1)
    fold = ((col == (lane >> 7) * 96 + (lane & 127)) & ((lane & 127) < 96)).astype(F32).astype(BF16)

    for h in range(2):
        rest = nn(perm, g[:, h, :, HALF:PACK].reshape(MAIN, HALF // 4)).astype(BF16)
        for b in range(4):
            xr[:, h * HALF + b * 384 : h * HALF + (b + 1) * 384] = rest[b * REST : (b + 1) * REST]

    def main_rows(h):
        return g[:, h, :, :HALF].reshape(MAIN, HALF)

    lt[:, :MAIN] = nt(w[:, :HALF], main_rows(0)) + nt(w[:, HALF:], main_rows(1))
    lt[:, MAIN:] = nt(w[...], xr[...])

    offset = ((z * 4 + xh * 2 + c) * SHARDS + me) * ROWS
    classes = offset + lax.broadcasted_iota(jnp.int32, (ROWS, TOK), 0)
    chosen = classes == labels[...]
    logits = lt[...]
    peak = jnp.max(logits, axis=0, keepdims=True)
    total = jnp.sum(jnp.exp(logits - peak), axis=0, keepdims=True)
    picked = jnp.sum(jnp.where(chosen, logits, 0.0), axis=0, keepdims=True)

    first = 0
    for devices in (peers[:7], peers[7:14], peers[14:]):
        phase = first // 7
        stat_send[phase, :, 0:TOK] = peak
        stat_send[phase, :, 384 : 384 + TOK] = total
        stat_send[phase, :, 768 : 768 + TOK] = picked
        for j, device in enumerate(devices):
            begin(copy(stat_send.at[phase], stat_recv.at[first + j], st_s.at[first + j], st_v.at[first + j], device))
        parts = [(peak, total, picked)]
        for j in range(7):
            arrived(stat_recv.at[first + j], st_s.at[first + j], st_v.at[first + j])
            parts.append((
                stat_recv[first + j, :, 0:TOK],
                stat_recv[first + j, :, 384 : 384 + TOK],
                stat_recv[first + j, :, 768 : 768 + TOK],
            ))
        peak = parts[0][0]
        for p in parts[1:]:
            peak = jnp.maximum(peak, p[0])
        total = sum(p[1] * jnp.exp(p[0] - peak) for p in parts)
        picked = sum(p[2] for p in parts)
        first += 7

    loss_out[...] = peak + jnp.log(total) - picked
    soft = jnp.exp(lt[...] - peak) / total
    gt[...] = (cot[...] * (soft - chosen.astype(F32))).astype(BF16)

    for k in range(RING):
        columns = slice(k * BLK, (k + 1) * BLK)
        main = tn(gt[:, :MAIN], w[:, columns]).astype(BF16).reshape(RING, 2, 16, BLK)
        pb[0, :, k] = main[..., :256]
        pb[1, k, :, :, :, 0:128] = main[..., 256:]
        rest = tn(gt[:, MAIN:], w[:, columns]).astype(BF16)
        folded = nn(rest, fold).astype(BF16)
        stacked = jnp.concatenate([folded[:, b * 128 : (b + 1) * 128] for b in range(4)], axis=0)
        pb[1, k, :, :, :, 128:256] = tn(perm, stacked).astype(BF16).reshape(RING, 2, 16, 128)

    pos = (1 - c) * y + c * z
    pos2 = (1 - c) * z + c * y

    def along(d):
        return {"dp_0": (y + (1 - c) * d) % RING, "cls_0": (z + c * d) % RING}

    def across(d):
        return {"dp_0": (y + c * d) % RING, "cls_0": (z + (1 - c) * d) % RING}

    for j in ORDER:
        begin(copy(pb.at[1 - c, (pos2 + j) % RING], rb.at[j], c_s.at[j], c_v.at[j], partner))

    def weight_part(h, lo, hi):
        at = slice(h * HALF + lo, h * HALF + hi)
        wg[:, at] = (
            nn(gt[:, :MAIN], g[:, h, :, lo:hi].reshape(MAIN, hi - lo)) + nn(gt[:, MAIN:], xr[:, at])
        ).astype(BF16)

    pieces = [(h, lo, lo + 384) for h in range(2) for lo in range(0, HALF, 384)]

    def mine(j, sub):
        s = slice(sub * 4, sub * 4 + 4)
        return pb[c, (pos + j) % RING, s].astype(F32) + rb[j, s].astype(F32)

    def hop(side, step, sub):
        s = pl.ds(sub * 4, 4)
        out, into = (send_r, recv_r) if side == 0 else (send_l, recv_l)
        return copy(out.at[step, s], into.at[step, s], rr_s.at[side, step, sub], rr_v.at[side, step, sub],
                    along(1 if side == 0 else -1))

    def landed(ref, step, side, sub):
        arrived(ref.at[step, pl.ds(sub * 4, 4)], rr_s.at[side, step, sub], rr_v.at[side, step, sub])

    for step in range(RIGHT):
        for side in range(2):
            steps = RIGHT if side == 0 else LEFT
            if step >= steps:
                continue
            j = steps - step if side == 0 else RING - (steps - step)
            arrived(rb.at[j], c_s.at[j], c_v.at[j])
            for sub in range(2):
                s = slice(sub * 4, sub * 4 + 4)
                value = mine(j, sub)
                if step:
                    ref = recv_r if side == 0 else recv_l
                    landed(ref, step - 1, side, sub)
                    value = value + ref[step - 1, s].astype(F32)
                (send_r if side == 0 else send_l)[step, s] = value.astype(BF16)
                begin(hop(side, step, sub))
        for piece in pieces[2 * step : 2 * step + 2]:
            weight_part(*piece)
    store_wg = pltpu.make_async_copy(wg, wg_out, wg_sem)
    store_wg.start()

    arrived(rb.at[0], c_s.at[0], c_v.at[0])
    for sub in range(2):
        s = slice(sub * 4, sub * 4 + 4)
        landed(recv_l, LEFT - 1, 1, sub)
        landed(recv_r, RIGHT - 1, 0, sub)
        value = mine(0, sub) + recv_l[LEFT - 1, s].astype(F32) + recv_r[RIGHT - 1, s].astype(F32)
        f32buf[s] = value
        f_send[s] = value.astype(BF16)
    for d in (4, 3, 5, 2, 6, 1, 7):
        begin(copy(f_send.at[(pos2 + d) % RING], f_recv.at[d - 1], f_s.at[d - 1], f_v.at[d - 1], across(d)))
    value = f32buf[pos2]
    for d in (1, 7, 2, 6, 3, 5, 4):
        arrived(f_recv.at[d - 1], f_s.at[d - 1], f_v.at[d - 1])
        value = value + f_recv[d - 1].astype(F32)

    s_send[...] = value
    for j, (dx, dc) in enumerate(others):
        begin(copy(s_send.at[(x + dx) % 2], s_recv.at[j], e_s.at[j], e_v.at[j], at_x(dx, dc)))
    same, other = s_send[xl], None
    for j, (dx, dc) in enumerate(others):
        arrived(s_recv.at[j], e_s.at[j], e_v.at[j])
        if dc == 0:
            same = same + s_recv[j]
        else:
            other = s_recv[j] if other is None else other + s_recv[j]
    hg_out[c] = same
    hg_out[1 - c] = other

    for d in sent:
        d.wait_send()
    store_wg.wait()


def body(hidden, weight, labels, cotangent):
    wide = hidden[:16].reshape(16, 2, HALF).transpose(1, 0, 2)
    rest = hidden[16:].reshape(4, 2, 4, HALF // 4).transpose(1, 2, 0, 3).reshape(2, 16, HALF // 4)
    packed = jnp.concatenate([wide, rest], axis=2)

    def reorder(v):
        v = v.reshape(SHARDS, 20)
        return jnp.concatenate([v[:, :16].reshape(1, MAIN), v[:, 16:].reshape(1, REST)], axis=1)

    vmem = pl.BlockSpec(memory_space=pltpu.VMEM)
    hbm = pl.BlockSpec(memory_space=pl.ANY)
    dma = pltpu.SemaphoreType.DMA
    loss, weight_grad, hg = pl.pallas_call(
        kernel,
        out_shape=(
            jax.ShapeDtypeStruct((1, TOK), F32),
            jax.ShapeDtypeStruct((ROWS, D), BF16),
            jax.ShapeDtypeStruct((2, 16, 256), F32),
        ),
        in_specs=[vmem, hbm, vmem, vmem],
        out_specs=(vmem, hbm, vmem),
        scratch_shapes=[
            pltpu.VMEM((ROWS, D), BF16),
            pltpu.VMEM((SHARDS, 2, 16, PACK), BF16),
            pltpu.VMEM((REST, D), BF16),
            pltpu.VMEM((ROWS, TOK), F32),
            pltpu.VMEM((ROWS, TOK), BF16),
            pltpu.VMEM((3, 1, 1152), F32),
            pltpu.VMEM((21, 1, 1152), F32),
            pltpu.VMEM((2, RING, RING, 2, 16, 256), BF16),
            pltpu.VMEM((RING, RING, 2, 16, 256), BF16),
            pltpu.VMEM((RIGHT, RING, 2, 16, 256), BF16),
            pltpu.VMEM((LEFT, RING, 2, 16, 256), BF16),
            pltpu.VMEM((RIGHT, RING, 2, 16, 256), BF16),
            pltpu.VMEM((LEFT, RING, 2, 16, 256), BF16),
            pltpu.VMEM((RING, 2, 16, 256), F32),
            pltpu.VMEM((RING, 2, 16, 256), BF16),
            pltpu.VMEM((RING - 1, 2, 16, 256), BF16),
            pltpu.VMEM((2, 16, 256), F32),
            pltpu.VMEM((7, 16, 256), F32),
            pltpu.VMEM((ROWS, D), BF16),
            dma, dma,
            dma((2, RIGHT, 2)), dma((2, RIGHT, 2)),
            dma((RING, 2)), dma((RING, 2)),
            dma((RING, 2, 2)), dma((RING, 2, 2)),
            dma((21,)), dma((21,)),
            dma((RING,)), dma((RING,)),
            dma((2, RIGHT, 2)), dma((2, RIGHT, 2)),
            dma((RING - 1,)), dma((RING - 1,)),
            dma((7,)), dma((7,)),
        ],
        compiler_params=pltpu.CompilerParams(
            collective_id=0, has_side_effects=True, vmem_limit_bytes=48 * 1024 * 1024
        ),
        name="step",
    )(packed, weight, reorder(labels), reorder(cotangent))

    me = lax.axis_index(DP)
    token_loss = jnp.concatenate([
        lax.dynamic_slice(loss[0], (me * 16,), (16,)),
        lax.dynamic_slice(loss[0], (MAIN + me * 4,), (4,)),
    ])
    block = lax.axis_index("cls_1") * 2 + lax.axis_index("cls_2")
    main = jnp.concatenate([hg[0], hg[1, :, :128]], axis=1)
    main = lax.dynamic_slice(main, (0, block * 96), (16, 96))
    rest = lax.dynamic_slice(hg[1], (block * 4, 128), (4, 96))
    hidden_grad = jnp.concatenate([main, rest], axis=0).astype(BF16)
    return (token_loss, weight_grad, hidden_grad)


def solution(mesh):
    torus = Mesh(mesh.devices.reshape(8, 2, 2, 8, 2), ("cls_0", "cls_1", "cls_2", "dp_0", "dp_1"))
    in_specs = (P(DP, None), P(CLS_DP, None), P(), P())
    out_specs = (P(DP), P(CLS_DP, None), P(DP, CLS))
    return jax.shard_map(body, mesh=torus, in_specs=in_specs, out_specs=out_specs, check_vma=False)
```

```python
import jax
import jax.numpy as jnp
from jax import lax
from jax.experimental import pallas as pl
from jax.experimental.pallas import tpu as pltpu
from jax.sharding import Mesh
from jax.sharding import PartitionSpec as P

CLS = ("cls_0", "cls_1", "cls_2")
DP = ("dp_0", "dp_1")
CLS_DP = ("cls_0", "cls_1", "cls_2", "dp_0", "dp_1")
MESH = pl.DeviceIdType.MESH
F32 = jnp.float32
BF16 = jnp.bfloat16

RING = 8
SHARDS = 16
D = 3072
ROWS = 384
TOK = 320
MAIN = 256
REST = 64
HALF = D // 2
PACK = HALF + HALF // 4
SUB = ((0, 1024), (1024, PACK - 1024))
BLK = 384
RIGHT = RING // 2
LEFT = RING - 1 - RIGHT
ORDER = (4, 5, 3, 6, 2, 7, 1, 0)


def nt(a, b):
    return lax.dot_general(a, b, (((1,), (1,)), ((), ())), preferred_element_type=F32)


def tn(a, b):
    return lax.dot_general(a, b, (((0,), (0,)), ((), ())), preferred_element_type=F32)


def nn(a, b):
    return lax.dot_general(a, b, (((1,), (0,)), ((), ())), preferred_element_type=F32)


def kernel(
    hid, w_hbm, labels, cot, loss_out, wg, hg_out,
    w, g, xr, lt, gt, per_token, stat_send, stat_recv, pb, rb, send_r, send_l, recv_r, recv_l,
    f32buf, f_send, f_recv, s_send, s_recv,
    w_sem, ring_s, ring_v, x_s, x_v, d_s, d_v, st_s, st_v, c_s, c_v, rr_s, rr_v, f_s, f_v, e_s, e_v,
):
    z, xh, c = lax.axis_index("cls_0"), lax.axis_index("cls_1"), lax.axis_index("cls_2")
    y, xl = lax.axis_index("dp_0"), lax.axis_index("dp_1")
    x = xh * 2 + xl
    me = y * 2 + xl

    def at_y(d):
        return {"dp_0": (y + d) % RING}

    def at_z(d):
        return {"cls_0": (z + d) % RING}

    def at_x(dx, dc):
        there = (x + dx) % 4
        return {"cls_1": there // 2, "dp_1": there % 2, "cls_2": (c + dc) % 2}

    partner = {"cls_2": 1 - c}

    def copy(src, dst, s, v, device):
        return pltpu.make_async_remote_copy(
            src_ref=src, dst_ref=dst, send_sem=s, recv_sem=v, device_id=device, device_id_type=MESH
        )

    load_w = pltpu.make_async_copy(w_hbm, w, w_sem)
    load_w.start()

    with jax.named_scope("barrier"):
        barrier = pltpu.get_barrier_semaphore()
        others = [(dx, dc) for dx in range(4) for dc in range(2) if dx or dc]
        peers = [at_x(dx, dc) for dx, dc in others]
        peers += [at_y(d) for d in range(1, RING)] + [at_z(d) for d in range(1, RING)]
        for peer in peers:
            pl.semaphore_signal(barrier, inc=1, device_id=peer, device_id_type=MESH)

        tail = hid[16:20].astype(F32)
        for h in range(2):
            g[me, h, :, :HALF] = hid[0:16, h * HALF : (h + 1) * HALF]
            base = h * HALF
            quarters = [tail[:, base + b * 384 : base + (b + 1) * 384] for b in range(4)]
            g[me, h, :, HALF:] = jnp.concatenate(quarters, axis=0).astype(BF16)
        pl.semaphore_wait(barrier, len(peers))

    sent = []

    def shard(o, own):
        return ((y + o) % RING) * 2 + (xl if own else 1 - xl)

    def part(o, own, h, sub):
        return g.at[shard(o, own), h, :, pl.ds(*SUB[sub])]

    def begin(d):
        d.start()
        sent.append(d)

    def ring(side, step, sub):
        o = -step if side == 0 else step
        begin(copy(part(o, True, c, sub), part(o, True, c, sub), ring_s.at[side, step, sub],
                   ring_v.at[side, step, sub], at_y(1 if side == 0 else -1)))

    def spread_x(o, sub):
        begin(copy(part(o, True, c, sub), part(o, True, c, sub), x_s.at[o % RING, sub],
                   x_v.at[o % RING, sub], at_x(1 if sub == 0 else 3, 0)))

    def spread_core(o, own, sub):
        begin(copy(part(o, own, c, sub), part(o, own, c, sub), d_s.at[o % RING, int(own), sub],
                   d_v.at[o % RING, int(own), sub], partner))

    def arrived(ref, s, v):
        copy(ref, ref, s, v, partner).wait_recv()

    with jax.named_scope("own"):
        for sub in range(2):
            ring(0, 0, sub)
            ring(1, 0, sub)
            spread_x(0, sub)

        lab, ct = labels[...], cot[...]
        ct_1 = ct.astype(BF16).astype(F32)
        ct_2 = (ct - ct_1).astype(BF16).astype(F32)
        rows = [(lab & 255).astype(F32), ((lab >> 8) & 255).astype(F32), (lab >> 16).astype(F32), ct_1, ct_2, ct - ct_1 - ct_2]
        per_token[...] = jnp.zeros_like(per_token)
        for k, row in enumerate(rows):
            per_token[k : k + 1] = row
        natural = lax.broadcasted_iota(jnp.int32, (TOK, TOK), 0)
        spot = lax.broadcasted_iota(jnp.int32, (TOK, TOK), 1)
        other = spot - MAIN
        holds = jnp.where(spot < MAIN, (spot >> 4) * 20 + (spot & 15), (other >> 2) * 20 + 16 + (other & 3))
        per_token[...] = nn(per_token[...].astype(BF16), (natural == holds).astype(F32).astype(BF16))

    def from_x(o):
        for sub in range(2):
            arrived(part(o, False, c, sub), x_s.at[o % RING, sub], x_v.at[o % RING, sub])
            spread_core(o, False, sub)

    with jax.named_scope("ring_gather"):
        waiting = [0]
        for step in range(RIGHT):
            got = []
            for sub in range(2):
                for side in range(2):
                    if side == 1 and step >= LEFT:
                        continue
                    o = -(step + 1) if side == 0 else step + 1
                    arrived(part(o, True, c, sub), ring_s.at[side, step, sub], ring_v.at[side, step, sub])
                    if step + 1 < (RIGHT if side == 0 else LEFT):
                        ring(side, step + 1, sub)
                    spread_x(o, sub)
                    spread_core(o, True, sub)
                    if sub == 1:
                        got.append(o)
            for o in waiting:
                from_x(o)
            waiting = got
        for o in waiting:
            from_x(o)
    with jax.named_scope("core_gather"):
        for o in [0] + [k for step in range(RIGHT) for k in (-(step + 1), step + 1)][: RING - 1]:
            for own in (True, False):
                if o == 0 and own:
                    continue
                for sub in range(2):
                    arrived(part(o, own, 1 - c, sub), d_s.at[o % RING, int(own), sub], d_v.at[o % RING, int(own), sub])
        load_w.wait()

    to = lax.broadcasted_iota(jnp.int32, (MAIN, MAIN), 0)
    source_row = lax.broadcasted_iota(jnp.int32, (MAIN, MAIN), 1)
    perm = (source_row == ((to & 63) >> 2) * 16 + (to >> 6) * 4 + (to & 3)).astype(F32).astype(BF16)
    col = lax.broadcasted_iota(jnp.int32, (BLK, 512), 0)
    lane = lax.broadcasted_iota(jnp.int32, (BLK, 512), 1)
    fold = ((col == (lane >> 7) * 96 + (lane & 127)) & ((lane & 127) < 96)).astype(F32).astype(BF16)

    with jax.named_scope("rest_rows"):
        for h in range(2):
            rest = nn(perm, g[:, h, :, HALF:PACK].reshape(MAIN, HALF // 4)).astype(BF16)
            for b in range(4):
                xr[:, h * HALF + b * 384 : h * HALF + (b + 1) * 384] = rest[b * REST : (b + 1) * REST]

    def main_rows(h):
        return g[:, h, :, :HALF].reshape(MAIN, HALF)

    with jax.named_scope("logits"):
        lt[:, :MAIN] = nt(w[:, :HALF], main_rows(0)) + nt(w[:, HALF:], main_rows(1))
        lt[:, MAIN:] = nt(w[...], xr[...])

    with jax.named_scope("local_stats"):
        offset = ((z * 4 + xh * 2 + c) * SHARDS + me) * ROWS
        classes = offset + lax.broadcasted_iota(jnp.int32, (ROWS, TOK), 0)
        label = per_token[0:1] + per_token[1:2] * 256.0 + per_token[2:3] * 65536.0
        chosen = classes == label.astype(jnp.int32)
        weight_of = per_token[3:4] + per_token[4:5] + per_token[5:6]
        logits = lt[...]
        peak = jnp.max(logits, axis=0, keepdims=True)
        total = jnp.sum(jnp.exp(logits - peak), axis=0, keepdims=True)
        picked = jnp.sum(jnp.where(chosen, logits, 0.0), axis=0, keepdims=True)

    with jax.named_scope("exchange"):
        first = 0
        for devices in (peers[:7], peers[7:14], peers[14:]):
            phase = first // 7
            stat_send[phase, :, 0:TOK] = peak
            stat_send[phase, :, 384 : 384 + TOK] = total
            stat_send[phase, :, 768 : 768 + TOK] = picked
            for j, device in enumerate(devices):
                begin(copy(stat_send.at[phase], stat_recv.at[first + j], st_s.at[first + j], st_v.at[first + j], device))
            parts = [(peak, total, picked)]
            for j in range(7):
                arrived(stat_recv.at[first + j], st_s.at[first + j], st_v.at[first + j])
                parts.append((
                    stat_recv[first + j, :, 0:TOK],
                    stat_recv[first + j, :, 384 : 384 + TOK],
                    stat_recv[first + j, :, 768 : 768 + TOK],
                ))
            peak = parts[0][0]
            for p in parts[1:]:
                peak = jnp.maximum(peak, p[0])
            total = sum(p[1] * jnp.exp(p[0] - peak) for p in parts)
            picked = sum(p[2] for p in parts)
            first += 7

    with jax.named_scope("grad"):
        loss_out[...] = peak + jnp.log(total) - picked
        soft = jnp.exp(lt[...] - peak) / total
        gt[...] = (weight_of * (soft - chosen.astype(F32))).astype(BF16)

    with jax.named_scope("partial"):
        for k in range(RING):
            columns = slice(k * BLK, (k + 1) * BLK)
            main = tn(gt[:, :MAIN], w[:, columns]).astype(BF16).reshape(RING, 2, 16, BLK)
            pb[0, :, k] = main[..., :256]
            pb[1, k, :, :, :, 0:128] = main[..., 256:]
            rest = tn(gt[:, MAIN:], w[:, columns]).astype(BF16)
            folded = nn(rest, fold).astype(BF16)
            stacked = jnp.concatenate([folded[:, b * 128 : (b + 1) * 128] for b in range(4)], axis=0)
            pb[1, k, :, :, :, 128:256] = tn(perm, stacked).astype(BF16).reshape(RING, 2, 16, 128)

    pos = (1 - c) * y + c * z
    pos2 = (1 - c) * z + c * y

    def along(d):
        return {"dp_0": (y + (1 - c) * d) % RING, "cls_0": (z + c * d) % RING}

    def across(d):
        return {"dp_0": (y + c * d) % RING, "cls_0": (z + (1 - c) * d) % RING}

    for j in ORDER:
        begin(copy(pb.at[1 - c, (pos2 + j) % RING], rb.at[j], c_s.at[j], c_v.at[j], partner))

    def weight_part(h, lo, hi):
        at = slice(h * HALF + lo, h * HALF + hi)
        wg[:, at] = (
            nn(gt[:, :MAIN], g[:, h, :, lo:hi].reshape(MAIN, hi - lo)) + nn(gt[:, MAIN:], xr[:, at])
        ).astype(BF16)

    pieces = [(h, lo, lo + 384) for h in range(2) for lo in range(0, HALF, 384)]

    def mine(j, sub):
        s = slice(sub * 4, sub * 4 + 4)
        return pb[c, (pos + j) % RING, s].astype(F32) + rb[j, s].astype(F32)

    def hop(side, step, sub):
        s = pl.ds(sub * 4, 4)
        out, into = (send_r, recv_r) if side == 0 else (send_l, recv_l)
        return copy(out.at[step, s], into.at[step, s], rr_s.at[side, step, sub], rr_v.at[side, step, sub],
                    along(1 if side == 0 else -1))

    def landed(ref, step, side, sub):
        arrived(ref.at[step, pl.ds(sub * 4, 4)], rr_s.at[side, step, sub], rr_v.at[side, step, sub])

    with jax.named_scope("ring_reduce"):
        for step in range(RIGHT):
            for side in range(2):
                steps = RIGHT if side == 0 else LEFT
                if step >= steps:
                    continue
                j = steps - step if side == 0 else RING - (steps - step)
                arrived(rb.at[j], c_s.at[j], c_v.at[j])
                for sub in range(2):
                    s = slice(sub * 4, sub * 4 + 4)
                    value = mine(j, sub)
                    if step:
                        ref = recv_r if side == 0 else recv_l
                        landed(ref, step - 1, side, sub)
                        value = value + ref[step - 1, s].astype(F32)
                    (send_r if side == 0 else send_l)[step, s] = value.astype(BF16)
                    begin(hop(side, step, sub))
            for piece in pieces[2 * step : 2 * step + 2]:
                weight_part(*piece)

    with jax.named_scope("ring_end"):
        arrived(rb.at[0], c_s.at[0], c_v.at[0])
        for sub in range(2):
            s = slice(sub * 4, sub * 4 + 4)
            landed(recv_l, LEFT - 1, 1, sub)
            landed(recv_r, RIGHT - 1, 0, sub)
            value = mine(0, sub) + recv_l[LEFT - 1, s].astype(F32) + recv_r[RIGHT - 1, s].astype(F32)
            f32buf[s] = value
            f_send[s] = value.astype(BF16)
    with jax.named_scope("across"):
        for d in (4, 3, 5, 2, 6, 1, 7):
            begin(copy(f_send.at[(pos2 + d) % RING], f_recv.at[d - 1], f_s.at[d - 1], f_v.at[d - 1], across(d)))
        value = f32buf[pos2]
        for d in (1, 7, 2, 6, 3, 5, 4):
            arrived(f_recv.at[d - 1], f_s.at[d - 1], f_v.at[d - 1])
            value = value + f_recv[d - 1].astype(F32)

    with jax.named_scope("last"):
        s_send[...] = value
        for j, (dx, dc) in enumerate(others):
            begin(copy(s_send.at[(x + dx) % 2], s_recv.at[j], e_s.at[j], e_v.at[j], at_x(dx, dc)))
        same, other = s_send[xl], None
        for j, (dx, dc) in enumerate(others):
            arrived(s_recv.at[j], e_s.at[j], e_v.at[j])
            if dc == 0:
                same = same + s_recv[j]
            else:
                other = s_recv[j] if other is None else other + s_recv[j]
        hg_out[c] = same
        hg_out[1 - c] = other

    with jax.named_scope("drain"):
        for d in sent:
            d.wait_send()


def body(hidden, weight, labels, cotangent):
    vmem = pl.BlockSpec(memory_space=pltpu.VMEM)
    hbm = pl.BlockSpec(memory_space=pltpu.HBM)
    dma = pltpu.SemaphoreType.DMA
    loss, weight_grad, hg = pl.pallas_call(
        kernel,
        out_shape=(
            jax.ShapeDtypeStruct((1, TOK), F32),
            jax.ShapeDtypeStruct((ROWS, D), BF16),
            jax.ShapeDtypeStruct((2, 16, 256), F32),
        ),
        in_specs=[vmem, hbm, vmem, vmem],
        out_specs=(vmem, vmem, vmem),
        scratch_shapes=[
            pltpu.VMEM((ROWS, D), BF16),
            pltpu.VMEM((SHARDS, 2, 16, PACK), BF16),
            pltpu.VMEM((REST, D), BF16),
            pltpu.VMEM((ROWS, TOK), F32),
            pltpu.VMEM((ROWS, TOK), BF16),
            pltpu.VMEM((8, TOK), F32),
            pltpu.VMEM((3, 1, 1152), F32),
            pltpu.VMEM((21, 1, 1152), F32),
            pltpu.VMEM((2, RING, RING, 2, 16, 256), BF16),
            pltpu.VMEM((RING, RING, 2, 16, 256), BF16),
            pltpu.VMEM((RIGHT, RING, 2, 16, 256), BF16),
            pltpu.VMEM((LEFT, RING, 2, 16, 256), BF16),
            pltpu.VMEM((RIGHT, RING, 2, 16, 256), BF16),
            pltpu.VMEM((LEFT, RING, 2, 16, 256), BF16),
            pltpu.VMEM((RING, 2, 16, 256), F32),
            pltpu.VMEM((RING, 2, 16, 256), BF16),
            pltpu.VMEM((RING - 1, 2, 16, 256), BF16),
            pltpu.VMEM((2, 16, 256), F32),
            pltpu.VMEM((7, 16, 256), F32),
            dma,
            dma((2, RIGHT, 2)), dma((2, RIGHT, 2)),
            dma((RING, 2)), dma((RING, 2)),
            dma((RING, 2, 2)), dma((RING, 2, 2)),
            dma((21,)), dma((21,)),
            dma((RING,)), dma((RING,)),
            dma((2, RIGHT, 2)), dma((2, RIGHT, 2)),
            dma((RING - 1,)), dma((RING - 1,)),
            dma((7,)), dma((7,)),
        ],
        compiler_params=pltpu.CompilerParams(
            collective_id=0, has_side_effects=True, vmem_limit_bytes=51 * 1024 * 1024
        ),
        name="step",
    )(hidden, weight, labels.reshape(1, TOK), cotangent.reshape(1, TOK))

    me = lax.axis_index(DP)
    token_loss = jnp.concatenate([
        lax.dynamic_slice(loss[0], (me * 16,), (16,)),
        lax.dynamic_slice(loss[0], (MAIN + me * 4,), (4,)),
    ])
    block = lax.axis_index("cls_1") * 2 + lax.axis_index("cls_2")
    main = jnp.concatenate([hg[0], hg[1, :, :128]], axis=1)
    main = lax.dynamic_slice(main, (0, block * 96), (16, 96))
    rest = lax.dynamic_slice(hg[1], (block * 4, 128), (4, 96))
    hidden_grad = jnp.concatenate([main, rest], axis=0).astype(BF16)
    return (token_loss, weight_grad, hidden_grad)


def solution(mesh):
    torus = Mesh(mesh.devices.reshape(8, 2, 2, 8, 2), ("cls_0", "cls_1", "cls_2", "dp_0", "dp_1"))
    in_specs = (P(DP, None), P(CLS_DP, None), P(), P())
    out_specs = (P(DP), P(CLS_DP, None), P(DP, CLS))
    return jax.shard_map(body, mesh=torus, in_specs=in_specs, out_specs=out_specs, check_vma=False)
```
